32 devices in a mesh: row: 4 (over y, x), col: 8 (over z, core).
Axes of the slice: x: 2, y: 2, z: 4, core: 2. Of those that a mesh axis runs over, the one named last changes fastest.
Arguments:
- inverse_state: float32 [8, 1024, 4, 2048], P(None, 'row', None, 'col')
- row_seeds: int32 [2, 8, 1024], P(None, None, 'row'), may hold values from 0 to 31
- col_seeds: int32 [2, 4, 2048], P(None, None, 'col'), may hold values from 0 to 31
Outputs:
- inverse: float32 [8, 1024, 4, 2048], P(None, 'row', None, 'col')
The draws below stay inside these ranges and needn't reach their ends.
All inputs are finite; a program needn't handle non-finite values.
Results may differ from the reference program's by a relative error of at most 0.0002.
Values sent between devices are 32-bit elements; how exact they have to be, the bound alone decides.
A program may use at most 64 MiB of HBM per device.

```python
import jax
import jax.numpy as jnp
from jax import lax

N = 8192
NB = 256
STEPS = 2
N_ROW = 4
N_COL = 8


def orthogonal_block(key):
    gauss = jax.random.normal(key, (NB, NB), jnp.float32)
    basis, upper = jnp.linalg.qr(gauss)
    return basis


def draw_inverse_state(key, part):
    key_base = jax.random.fold_in(key, 11)
    base = jax.random.normal(key_base, (N, N), jnp.float32)
    low_end = 2.0 * jnp.sqrt(jnp.float32(NB))
    high_end = 4.0 * low_end
    for step in range(STEPS):
        key_sing = jax.random.fold_in(key, 100 + step)
        key_left = jax.random.fold_in(key, 200 + step)
        key_right = jax.random.fold_in(key, 300 + step)
        singular = jnp.exp(jax.random.uniform(key_sing, (NB,), jnp.float32, 0.0, 1.0) * jnp.log(high_end / low_end)) * low_end
        left_basis = orthogonal_block(key_left)
        right_basis = orthogonal_block(key_right)
        pivot = jnp.dot(left_basis * singular[None, :], right_basis.T, precision=lax.Precision.HIGHEST, preferred_element_type=jnp.float32)
        start = N - (STEPS - step) * NB
        base = base.at[start:start + NB, start:start + NB].set(pivot)
    return base.reshape(N // (N_ROW * NB), N_ROW * NB, N // (N_COL * NB), N_COL * NB)


def place_ends(values, stream_key, low, high):
    dims = values.shape
    index_at = [jax.random.randint(jax.random.fold_in(stream_key, axis), (), 0, dims[axis]) for axis in range(len(dims))]
    values = values.at[tuple(index_at)].set(low)
    longest = dims.index(max(dims))
    index_at[longest] = (index_at[longest] + 1) % dims[longest]
    return values.at[tuple(index_at)].set(high)


def setup_inputs(seed: int = 0) -> dict:
    keys = jax.random.split(jax.random.key(seed), 4)
    return {
        "inverse_state": draw_inverse_state(jax.random.fold_in(keys[3], 71), 0),
        "row_seeds": place_ends(jax.random.randint(keys[1], (2, N // (N_ROW * NB), N_ROW * NB), 0, 32), jax.random.fold_in(keys[1], 1), 0, 31).astype(jnp.int32),
        "col_seeds": place_ends(jax.random.randint(keys[2], (2, N // (N_COL * NB), N_COL * NB), 0, 32), jax.random.fold_in(keys[2], 1), 0, 31).astype(jnp.int32),
    }


root_half = 0.7071067811865476

def level_apply(matrix, scales, groups):
    count = matrix.shape[0]
    half = count // (2 * groups)
    shaped = matrix.reshape(groups, 2, half, matrix.shape[1])
    factor = scales.reshape(groups, 2, half, 1)
    upper = factor[:, 0] * shaped[:, 0]
    lower = factor[:, 1] * shaped[:, 1]
    return (jnp.stack([upper + lower, upper - lower], axis=1) * root_half).reshape(matrix.shape)

def butterfly(matrix, seeds):
    scales = (2.0 * seeds.reshape(2, N).astype(jnp.float32) - 31.0) / 16.0
    return level_apply(level_apply(matrix, scales[0], 1), scales[1], 2)

def reference(inverse_state, row_seeds, col_seeds):
    matrix = inverse_state.reshape(N, N)
    identity = jnp.eye(NB, dtype=jnp.float32)
    for step in range(STEPS):
        start = N - (STEPS - step) * NB
        stop = start + NB
        pivot = matrix[start:stop, start:stop]
        shifted = matrix.at[:, start:stop].set(0.0)
        shifted = shifted.at[start:stop, start:stop].set(identity)
        right_part = jnp.linalg.solve(pivot, shifted[start:stop])
        left_part = matrix[:, start:stop].at[start:stop].set(pivot - identity)
        matrix = shifted - jnp.dot(left_part.astype(jnp.float32), right_part.astype(jnp.float32), precision=lax.Precision.HIGHEST, preferred_element_type=jnp.float32)
    rows_done = butterfly(matrix, row_seeds)
    result = butterfly(rows_done.T, col_seeds).T
    return result.reshape(inverse_state.shape)
```

```python
import functools

import jax
import jax.numpy as jnp
from jax import lax
from jax.experimental import pallas as pl
from jax.experimental.pallas import tpu as pltpu
from jax.sharding import PartitionSpec as P

STEPS = 2
LANES = 128
root_half = 0.7071067811865476
HIGHEST = lax.Precision.HIGHEST
VMEM_BYTES = 60 * 1024 * 1024


def swapped(block, axis, bit):
    count = lax.axis_size(axis)
    route = []
    for low in range(count):
        high = low | 1 << bit
        if high != low and high < count:
            route += [(low, high), (high, low)]
    return lax.ppermute(block, axis, route)


def seed_values(seeds):
    return (2.0 * seeds.astype(jnp.float32) - 31.0) / 16.0


def col_level(matrix, scales, groups, mover, col_index, span):
    if mover is None:
        count = matrix.shape[1]
        half = count // (2 * groups)
        shaped = matrix.reshape(matrix.shape[0], groups, 2, half, matrix.shape[2])
        factor = scales.reshape(groups, 2, half, scales.shape[1])
        upper = factor[:, 0] * shaped[:, :, 0]
        lower = factor[:, 1] * shaped[:, :, 1]
        return (jnp.stack([upper + lower, upper - lower], axis=2) * root_half).reshape(matrix.shape)
    own_part = scales * matrix
    partner = mover(own_part)
    on_top = col_index // span % 2 == 0
    return jnp.where(on_top, own_part + partner, partner - own_part) * root_half


def col_butterfly(matrix, seeds):
    scales = seed_values(seeds)
    col_count = lax.axis_size("col")
    col_index = lax.axis_index("col")
    blocks_all = matrix.shape[1] * col_count
    for level, groups in ((0, 1), (1, 2)):
        span = blocks_all // (2 * groups)
        bit = span.bit_length() - 1
        mover = None if span % col_count == 0 else lambda values: swapped(values, "col", bit)
        matrix = col_level(matrix, scales[level], groups, mover, col_index, span)
    return matrix


def levels(parts, first, second):
    count = len(parts)
    for scales, groups in ((first, 1), (second, 2)):
        half = count // (2 * groups)
        done = list(parts)
        for group in range(groups):
            for at in range(half):
                top = group * 2 * half + at
                low = top + half
                upper = scales[top] * parts[top]
                lower = scales[low] * parts[low]
                done[top] = upper + lower
                done[low] = upper - lower
        parts = done
    return parts


def split(x):
    high = x.astype(jnp.bfloat16)
    return high, (x - high.astype(jnp.float32)).astype(jnp.bfloat16)


def dot_f32(a, b):
    return jnp.dot(a, b, precision=HIGHEST, preferred_element_type=jnp.float32)


def dot_split(a, b):
    a_high, a_low = split(a)
    b_high, b_low = split(b)
    dot = functools.partial(jnp.dot, preferred_element_type=jnp.float32)
    return dot(a_high, b_high) + dot(a_high, b_low) + dot(a_low, b_high)


def eye_of(rows, columns, row_start=0, column_start=0):
    at_row = lax.broadcasted_iota(jnp.int32, (rows, columns), 0) + row_start
    at_column = lax.broadcasted_iota(jnp.int32, (rows, columns), 1) + column_start
    return jnp.where(at_row == at_column, 1.0, 0.0).astype(jnp.float32)


def extract_kernel(row_blocks, col_blocks, block, x_ref, c_ref, r_ref):
    stride = col_blocks * (block // LANES)

    def piece(b, h):
        return x_ref[pl.ds(h * col_blocks + b, block, stride=stride), :]

    for h in range(block // LANES):
        c_ref[0, :, h * LANES:(h + 1) * LANES] = piece(col_blocks - 1, h)

    @pl.when(pl.program_id(0) == row_blocks - 1)
    def _():
        for b in range(col_blocks):
            for h in range(block // LANES):
                start = b * block + h * LANES
                r_ref[:, start:start + LANES] = piece(b, h)


def spread_kernel(
    chunk_count, piece_count, col_count, row_count,
    c_ref, r_ref, cpan, rpan, ppan,
    c_down, c_down_in, c_mate, c_mate_in,
    r_down, r_down_in, r_mate, r_mate_in,
    p_down, p_down_in, p_mate, p_mate_in, p_core, p_core_in, local,
):
    row_blocks, block, _ = c_ref.shape
    col, row = lax.axis_index("col"), lax.axis_index("row")
    k, j = lax.rem(col, 2), lax.rem(row, 2)
    col_mate, row_mate = col + 1 - 2 * k, row + 1 - 2 * j
    col_root, row_root = col >= col_count - 2, row >= row_count - 2
    col_has, row_has = col >= 2, row >= 2
    col_low, row_low = jnp.maximum(col - 2, 0), jnp.maximum(row - 2, 0)
    col_up = jnp.minimum(col + 2, col_count - 1)
    row_up = jnp.minimum(row + 2, row_count - 1)

    barrier = pltpu.get_barrier_semaphore()

    def greet(axis, target):
        pl.semaphore_signal(
            barrier, inc=1, device_id={axis: target}, device_id_type=pl.DeviceIdType.MESH
        )

    greet("col", col_mate)
    greet("row", row_mate)
    pl.when(col_has)(lambda: greet("col", col_low))
    pl.when(row_has)(lambda: greet("row", row_low))
    pl.when(jnp.logical_not(col_root))(lambda: greet("col", col_up))
    pl.when(jnp.logical_not(row_root))(lambda: greet("row", row_up))
    peers = 4 - col_root.astype(jnp.int32) - row_root.astype(jnp.int32)
    peers = peers + col_has.astype(jnp.int32) + row_has.astype(jnp.int32)
    pl.semaphore_wait(barrier, peers)

    def remote(src, dst, send, receive, axis, target):
        return pltpu.make_async_remote_copy(
            src_ref=src, dst_ref=dst, send_sem=send, recv_sem=receive,
            device_id={axis: target}, device_id_type=pl.DeviceIdType.MESH,
        )

    own_c = pltpu.make_async_copy(c_ref, cpan.at[k], local.at[0])
    own_r = pltpu.make_async_copy(r_ref, rpan.at[j], local.at[1])
    own_p = pltpu.make_async_copy(cpan.at[k, row_blocks - 1], ppan.at[k, j], local.at[2])
    pl.when(col_root)(own_c.start)
    pl.when(row_root)(own_r.start)
    pl.when(col_root)(own_c.wait)
    pl.when(row_root)(own_r.wait)

    per_block = chunk_count // row_blocks
    rows_each = block // per_block

    def c_at(side, index):
        a = row_blocks - 1 - index // per_block
        return cpan.at[side, a, pl.ds(index % per_block * rows_each, rows_each), :]

    def c_step(index):
        down = remote(c_at(k, index), c_at(k, index), c_down.at[index], c_down_in.at[index], "col", col_low)
        mate = remote(c_at(k, index), c_at(k, index), c_mate.at[index], c_mate_in.at[index], "col", col_mate)
        pl.when(jnp.logical_not(col_root))(down.wait_recv)
        pl.when(col_has)(down.start)
        mate.start()
        return down, mate

    piece_rows = block // piece_count

    def r_at(side, index):
        return rpan.at[side, pl.ds(index * piece_rows, piece_rows), :]

    def r_step(index):
        down = remote(r_at(j, index), r_at(j, index), r_down.at[index], r_down_in.at[index], "row", row_low)
        mate = remote(r_at(j, index), r_at(j, index), r_mate.at[index], r_mate_in.at[index], "row", row_mate)
        pl.when(jnp.logical_not(row_root))(down.wait_recv)
        pl.when(row_has)(down.start)
        mate.start()
        return down, mate

    c_copies, r_copies = [], []
    for index in range(per_block):
        c_copies.append(c_step(index))

    p_low = remote(ppan.at[k, j], ppan.at[k, j], p_down, p_down_in, "row", row_low)
    p_side = remote(ppan.at[k, j], ppan.at[k, j], p_mate, p_mate_in, "row", row_mate)
    p_over = remote(ppan.at[k], ppan.at[k], p_core, p_core_in, "col", col_mate)

    pl.when(row_root)(own_p.start)
    pl.when(row_root)(own_p.wait)
    pl.when(jnp.logical_not(row_root))(p_low.wait_recv)
    pl.when(row_has)(p_low.start)
    p_side.start()

    done = 0
    for index in range(per_block, chunk_count):
        c_copies.append(c_step(index))
        wanted = min(piece_count, index - per_block + 1)
        while done < wanted:
            r_copies.append(r_step(done))
            done += 1
    while done < piece_count:
        r_copies.append(r_step(done))
        done += 1
    p_side.wait_recv()
    p_over.start()

    for down, mate in c_copies:
        mate.wait_recv()
        mate.wait_send()
        pl.when(col_has)(down.wait_send)
    for down, mate in r_copies:
        mate.wait_recv()
        mate.wait_send()
        pl.when(row_has)(down.wait_send)
    p_side.wait_send()
    pl.when(row_has)(p_low.wait_send)
    p_over.wait_recv()
    p_over.wait_send()


def inverse_of(matrix, cap=60):
    size = matrix.shape[0]
    identity = eye_of(size, size)
    matrix_t = matrix.T
    gram = dot_split(matrix_t, matrix)
    bound = jnp.max(jnp.sum(jnp.abs(gram), axis=0, keepdims=True))
    guess = matrix_t * (1.8 / bound)

    def going(carry):
        count, _, worst, before = carry
        return jnp.logical_and(
            count < cap,
            jnp.logical_or(worst > 1e-2, jnp.logical_and(worst > 1e-6, worst < 0.5 * before)),
        )

    def body(carry):
        count, x, worst, _ = carry
        error = identity - dot_f32(matrix, x)
        x = x + dot_split(x, error)
        return count + 1, x, jnp.max(jnp.abs(error)), worst

    start = (jnp.int32(0), guess, jnp.float32(1e30), jnp.float32(1e30))
    return lax.while_loop(going, body, start)[1]


def solve_kernel(col_blocks, block, local_cols, flags, p_ref, r_ref, d_ref, high_ref, low_ref):
    a11, a21 = p_ref[0, 0], p_ref[0, 1]
    a12, a22 = p_ref[1, 0], p_ref[1, 1]
    last = (col_blocks - 1) * block
    identity = eye_of(block, block)
    for step in range(STEPS):
        here = jnp.where(flags[1] == step, identity, jnp.zeros_like(identity))

        @pl.when(flags[0] == 1)
        def _():
            r_ref[step, :, last:] = here

    first_inverse = inverse_of(a11)
    low_left = dot_f32(a21, first_inverse)
    second_inverse = inverse_of(a22 - dot_f32(low_left, a12))
    right = dot_f32(second_inverse, r_ref[1] - dot_f32(low_left, r_ref[0]))
    left = dot_f32(first_inverse, r_ref[0] - dot_f32(a12, right))
    for step, value in ((0, left), (1, right)):
        parts = [value[:, b * block:(b + 1) * block] for b in range(col_blocks)]
        if local_cols:
            scales = [
                [d_ref[level:level + 1, b * block:(b + 1) * block] for b in range(col_blocks)]
                for level in range(2)
            ]
            parts = levels(parts, *scales)
        for b, part in enumerate(parts):
            high, low = split(part)
            high_ref[step * block:(step + 1) * block, b * block:(b + 1) * block] = high
            low_ref[step * block:(step + 1) * block, b * block:(b + 1) * block] = low


def final_kernel(
    row_blocks, col_blocks, block, tile, local_cols, flags,
    x_ref, c_ref, rd_ref, cd_ref, high_ref, low_ref, out_ref, left_high, left_low, product,
):
    halves = block // LANES
    stride = col_blocks * halves
    start = pl.program_id(0) * tile
    row_scales = [
        [rd_ref[:, level * row_blocks + a:level * row_blocks + a + 1] for a in range(row_blocks)]
        for level in range(2)
    ]
    for step in range(STEPS):
        for h in range(halves):
            lanes = pl.ds(h * LANES, LANES)
            parts = [c_ref[step, a, :, lanes] for a in range(row_blocks)]
            parts[-1] = parts[-1] - jnp.where(
                flags[2] == step, eye_of(tile, LANES, start, h * LANES), 0.0
            )
            for a, part in enumerate(levels(parts, *row_scales)):
                high, low = split(part)
                place = (pl.ds(a * tile, tile), pl.ds(step * block + h * LANES, LANES))
                left_high[place] = high
                left_low[place] = low
    dot = functools.partial(jnp.dot, preferred_element_type=jnp.float32)
    for b in range(col_blocks):
        at = pl.ds(b * block, block)
        product[:, at] = (
            dot(left_high[...], high_ref[:, at])
            + dot(left_high[...], low_ref[:, at])
            + dot(left_low[...], high_ref[:, at])
        )
    for h in range(halves):
        columns = []
        for b in range(col_blocks):
            at = pl.ds(h * col_blocks + b, tile, stride=stride)
            parts = [x_ref[a, at, :] for a in range(row_blocks)]
            if b == col_blocks - 1:
                parts = [jnp.where(flags[0] == 1, 0.0, part) for part in parts]
                parts[-1] = parts[-1] + jnp.where(
                    flags[3] == 1, eye_of(tile, LANES, start, h * LANES), 0.0
                )
            columns.append(levels(parts, *row_scales))
        for a in range(row_blocks):
            parts = [columns[b][a] for b in range(col_blocks)]
            if local_cols:
                scales = [
                    [
                        cd_ref[level:level + 1, b * block + h * LANES:b * block + (h + 1) * LANES]
                        for b in range(col_blocks)
                    ]
                    for level in range(2)
                ]
                parts = levels(parts, *scales)
            for b in range(col_blocks):
                at = pl.ds(h * col_blocks + b, tile, stride=stride)
                spot = b * block + h * LANES
                out_ref[a, at, :] = parts[b] - product[a * tile:(a + 1) * tile, spot:spot + LANES]


def per_device(inverse_state, row_seeds, col_seeds):
    row_blocks, block, col_blocks, _ = inverse_state.shape
    row_count, col_count = lax.axis_size("row"), lax.axis_size("col")
    halves = block // LANES
    lines = block * halves * col_blocks
    width = col_blocks * block
    local_cols = col_blocks % 4 == 0
    f32 = jnp.float32
    vmem = pl.BlockSpec(memory_space=pltpu.VMEM)
    smem = pl.BlockSpec(memory_space=pltpu.SMEM)
    params = functools.partial(pltpu.CompilerParams, vmem_limit_bytes=VMEM_BYTES)

    native = inverse_state.reshape(row_blocks, block, col_blocks, halves, LANES)
    native = native.transpose(0, 1, 3, 2, 4).reshape(row_blocks, lines, LANES)
    row, col = lax.axis_index("row"), lax.axis_index("col")
    row_step, col_step = row - (row_count - STEPS), col - (col_count - STEPS)
    flags = jnp.stack([
        col_step >= 0, col_step, row_step, jnp.logical_and(col_step >= 0, col_step == row_step),
    ]).astype(jnp.int32)
    row_scales = (seed_values(row_seeds) * root_half).reshape(2 * row_blocks, block).T
    col_scales = (seed_values(col_seeds) * root_half).reshape(2, width)

    column, pivot_rows = pl.pallas_call(
        functools.partial(extract_kernel, row_blocks, col_blocks, block),
        grid=(row_blocks,),
        in_specs=[pl.BlockSpec((None, lines, LANES), lambda a: (a, 0, 0))],
        out_specs=[
            pl.BlockSpec((1, block, block), lambda a: (a, 0, 0)),
            pl.BlockSpec((block, width), lambda a: (0, 0)),
        ],
        out_shape=[
            jax.ShapeDtypeStruct((row_blocks, block, block), f32),
            jax.ShapeDtypeStruct((block, width), f32),
        ],
        name="extract",
        compiler_params=params(),
    )(native)

    chunks, pieces = 2 * row_blocks, 4
    dma = pltpu.SemaphoreType.DMA
    panel, rows, pivot = pl.pallas_call(
        functools.partial(spread_kernel, chunks, pieces, col_count, row_count),
        in_specs=[vmem, vmem],
        out_specs=[vmem, vmem, vmem],
        out_shape=[
            jax.ShapeDtypeStruct((STEPS, row_blocks, block, block), f32),
            jax.ShapeDtypeStruct((STEPS, block, width), f32),
            jax.ShapeDtypeStruct((STEPS, STEPS, block, block), f32),
        ],
        scratch_shapes=[dma((chunks,))] * 4 + [dma((pieces,))] * 4 + [dma] * 6 + [dma((3,))],
        name="spread",
        compiler_params=params(collective_id=0, has_side_effects=True),
    )(column, pivot_rows)

    high, low = pl.pallas_call(
        functools.partial(solve_kernel, col_blocks, block, local_cols),
        in_specs=[smem, vmem, vmem, vmem],
        out_specs=[vmem, vmem],
        out_shape=[jax.ShapeDtypeStruct((STEPS * block, width), jnp.bfloat16)] * 2,
        name="solve",
        compiler_params=params(),
    )(flags, pivot, rows, col_scales)

    tile = block // 4
    whole = lambda i: (0, 0)
    out = pl.pallas_call(
        functools.partial(final_kernel, row_blocks, col_blocks, block, tile, local_cols),
        grid=(block // tile,),
        in_specs=[
            smem,
            pl.BlockSpec((row_blocks, lines // 4, LANES), lambda i: (0, i, 0)),
            pl.BlockSpec((STEPS, row_blocks, tile, block), lambda i: (0, 0, i, 0)),
            pl.BlockSpec((tile, 2 * row_blocks), lambda i: (i, 0)),
            pl.BlockSpec((2, width), whole),
            pl.BlockSpec((STEPS * block, width), whole),
            pl.BlockSpec((STEPS * block, width), whole),
        ],
        out_specs=pl.BlockSpec((row_blocks, lines // 4, LANES), lambda i: (0, i, 0)),
        out_shape=jax.ShapeDtypeStruct((row_blocks, lines, LANES), f32),
        scratch_shapes=[
            pltpu.VMEM((row_blocks * tile, STEPS * block), jnp.bfloat16),
            pltpu.VMEM((row_blocks * tile, STEPS * block), jnp.bfloat16),
            pltpu.VMEM((row_blocks * tile, width), f32),
        ],
        name="final",
        compiler_params=params(),
    )(flags, native, panel, row_scales, col_scales, high, low)
    out = out.reshape(row_blocks, block, halves, col_blocks, LANES).transpose(0, 1, 3, 2, 4)
    out = out.reshape(inverse_state.shape)
    if not local_cols:
        flat = out.reshape(row_blocks * block, col_blocks, block)
        out = col_butterfly(flat, col_seeds).reshape(inverse_state.shape)
    return out


def solution(mesh):
    placed = (P(None, "row", None, "col"), P(None, None, "row"), P(None, None, "col"))
    return jax.shard_map(
        per_device,
        mesh=mesh,
        in_specs=placed,
        out_specs=P(None, "row", None, "col"),
        check_vma=False,
    )
```
